256 devices in a mesh: gx: 4 (over z_lo), gy: 4 (over y), gz: 16 (over x, z_hi, core).
Axes of the slice: x: 4, y: 4, z: 8 (z_hi: 2, z_lo: 4; z = z_hi * 4 + z_lo), core: 2. Of those that a mesh axis runs over, the one named last changes fastest.
Arguments:
- factor_inv: bfloat16 [4, 4096, 16384], P('gx', 'gy', 'gz')
- sep_sizes: int32 [4, 4, 16], P('gx', 'gy', 'gz'), may hold values from 512 to 1024
- coupling: bfloat16 [12, 4096, 16384], P('gx', 'gy', 'gz'), may hold values from -0.109375 to 0.109375
Outputs:
- schur_update: float32 [4, 4096, 16384], P('gx', 'gy', 'gz')
The draws below stay inside these ranges and needn't reach their ends.
All inputs are finite; a program needn't handle non-finite values.
Results may differ from the reference program's by a relative error of at most 0.0023.
Values may be sent and summed in bfloat16 or wider, within the bound.
A program may use at most 128 MiB of HBM per device.

```python
import jax
import jax.numpy as jnp
from jax import lax

W = 1024
M = 1024
SLOTS = 3
N_GX = 4
N_GY = 4
N_GZ = 16


def draw_factor_inv(key, part):
    first, second = jax.random.split(jax.random.fold_in(key, 11))
    shape = (N_GX, N_GY * W, N_GZ * W)
    rows = lax.broadcasted_iota(jnp.int32, shape, 1) % W
    cols = lax.broadcasted_iota(jnp.int32, shape, 2) % W
    lower = jax.random.normal(first, shape, jnp.float32)
    diag = jax.random.uniform(second, shape, jnp.float32, 0.5, 1.5)
    scaled = lower / jnp.sqrt(jnp.float32(W))
    return jnp.where(rows > cols, scaled, jnp.where(rows == cols, diag, jnp.float32(0.0))).astype(jnp.bfloat16)


def with_ends(entries, key, smallest, high):
    shape = entries.shape
    index_at = [jax.random.randint(jax.random.fold_in(key, axis), (), 0, shape[axis]) for axis in range(len(shape))]
    entries = entries.at[tuple(index_at)].set(smallest)
    longest = shape.index(max(shape))
    index_at[longest] = (index_at[longest] + 1) % shape[longest]
    return entries.at[tuple(index_at)].set(high)


def level_of(own_key, extent, cuts, low, largest):
    def one(dim, blocks):
        steps = jax.random.uniform(jax.random.fold_in(jax.random.fold_in(own_key, 6), dim), (blocks,), jnp.float32, low / len(cuts), largest / len(cuts))
        return jnp.repeat(jnp.exp(steps), extent[dim] // blocks).reshape((-1,) + (1,) * (len(extent) - dim - 1))

    gain = one(*cuts[0])
    for cut in cuts[1:]:
        gain = gain * one(*cut)
    return gain


def gaussian(key, dims, spread, most, cuts=(), held_as=jnp.bfloat16):
    drawn = jax.random.normal(key, dims, jnp.float32) * spread
    if len(cuts) > 0:
        drawn = level_of(key, dims, cuts, -0.22, 0.18) * drawn
    return jnp.clip(drawn, min=-most, max=most).astype(held_as)


def setup_inputs(seed: int = 0) -> dict:
    splits = jax.random.split(jax.random.key(seed), 4)
    factor_inv = draw_factor_inv(jax.random.fold_in(splits[3], 71), 0)
    sep_sizes = with_ends(jax.random.randint(splits[1], (N_GX, N_GY, N_GZ), W // 2, W + 1), jax.random.fold_in(splits[1], 1), W // 2, W).astype(jnp.int32)
    coupling = gaussian(splits[2], (N_GX * SLOTS, N_GY * W, N_GZ * M), (3 * W) ** -0.5, 0.109375, ((0, 4), (1, 4), (2, 16)))
    return dict(factor_inv=factor_inv, sep_sizes=sep_sizes, coupling=coupling)


def reference(factor_inv, sep_sizes, coupling):
    nxa = factor_inv.shape[0]
    nya = factor_inv.shape[1] // W
    nza = factor_inv.shape[2] // W
    inner = jnp.arange(W, dtype=jnp.int32)

    def owned(iidx, jidx, kidx):
        valid = (jidx >= 0) & (jidx < nya) & (kidx >= 0) & (kidx < nza)
        jc = jnp.clip(jidx, 0, nya - 1).astype(jnp.int32)
        kc = jnp.clip(kidx, 0, nza - 1).astype(jnp.int32)
        block = lax.dynamic_slice(factor_inv, (iidx, jc * W, kc * W), (1, W, W))[0]
        count = lax.dynamic_slice(sep_sizes, (iidx, jc, kc), (1, 1, 1))[0, 0, 0]
        keep = ((inner < count) & valid).astype(jnp.bfloat16)
        return block * keep[:, None] * keep[None, :]

    def one(flat):
        iidx = (flat // (nya * nza)).astype(jnp.int32)
        jidx = ((flat // nza) % nya).astype(jnp.int32)
        kidx = (flat % nza).astype(jnp.int32)
        cblock = lax.dynamic_slice(coupling, (iidx * 3, jidx * W, kidx * M), (3, W, M))
        factors = [owned(iidx, jidx, kidx - 1), owned(iidx, jidx, kidx + 1), owned(iidx, jidx - 1, kidx)]
        total = jnp.zeros((M, M), jnp.float32)
        for slot in range(3):
            solved = jnp.dot(factors[slot], cblock[slot], preferred_element_type=jnp.float32).astype(jnp.bfloat16)
            total = total + jnp.dot(solved.T, solved, preferred_element_type=jnp.float32)
        return total

    result = lax.map(one, jnp.arange(nxa * nya * nza, dtype=jnp.int32))
    result = result.reshape(nxa, nya, nza, M, M).transpose(0, 1, 3, 2, 4)
    return result.reshape(nxa, nya * M, nza * M)
```

```python
import jax
import jax.numpy as jnp
from jax import lax
from jax.experimental import pallas as pl
from jax.experimental.pallas import tpu as pltpu
from jax.sharding import PartitionSpec as P

MESH = pl.DeviceIdType.MESH
BF = jnp.bfloat16
F32 = jnp.float32
B = 256
CROSS, PARTNER, BELOW = 0, 1, 2
SMALL = 4
TN = (((0,), (0,)), ((), ()))


def tri(shape):
    return lax.broadcasted_iota(jnp.int32, shape, 0), lax.broadcasted_iota(jnp.int32, shape, 1)


def gram_rows(g, u):
    return lax.dot_general(g[:, u * B:(u + 1) * B], g[:, u * B:], TN, preferred_element_type=F32)


def packed(lower, upper):
    row, col = tri((B, B))
    return jnp.where(row > col, lower, jnp.where(row == col, 0.5 * upper, upper))


def half_diagonal(block):
    row, col = tri((B, B))
    return jnp.sum(jnp.where(row == col, 0.5 * block, 0.0), axis=0, keepdims=True)


def exchange(f_hbm, n_ref, c_hbm, t_ref, g, c, z, half, left, right, sbuf, ssmall, rbuf, rsmall, pbuf,
             sems, send_sem, recv_sem, small_send, small_recv, pass_send, pass_recv):
    zlo, y, gz = lax.axis_index("gx"), lax.axis_index("gy"), lax.axis_index("gz")
    size_y, size_z = lax.axis_size("gy"), lax.axis_size("gz")
    core, x, kind = lax.rem(gz, 2), gz // 4, lax.rem(gz, 4)
    partner = gz + 1 - 2 * core
    cross = gz - 1 + 2 * core
    has_cross = (cross >= 0) & (cross < size_z)
    has_up, has_below = y < size_y - 1, y > 0

    steps = size_z // 4
    outer = (kind == 3) | (kind == 0)
    forward = kind == 3
    has_right, has_left = outer & (x < steps - 1), outer & (x > 0)
    n_passed = jnp.where(has_cross & outer, jnp.where(forward, x + 1, steps - x), 0)
    n_passing = jnp.where(outer, jnp.where(forward, x, steps - 1 - x), 0)
    passer = gz + jnp.where(forward, 4, -4)
    receiver = gz + jnp.where(forward, -3, 3)

    def at(col, row=None):
        row = y if row is None else jnp.clip(row, 0, size_y - 1)
        return (zlo, row, jnp.clip(col, 0, size_z - 1))

    sends_to = {CROSS: at(cross), PARTNER: at(partner), BELOW: at(gz, y + 1)}
    sends = {CROSS: has_cross, PARTNER: gz >= 0, BELOW: has_up}
    gets = {CROSS: has_cross, PARTNER: gz >= 0, BELOW: has_below}
    slot_of = {CROSS: core, PARTNER: 1 - core, BELOW: 2}

    load_f = pltpu.make_async_copy(f_hbm.at[0], g, sems.at[0])
    load_f.start()

    barrier = pltpu.get_barrier_semaphore()
    peers = [(has_cross, at(cross)), (outer, at(receiver)), (has_right, at(gz + 4)), (has_left, at(gz - 4)),
             (has_up, at(gz, y + 1)), (has_below, at(gz, y - 1)), (gz >= 0, at(partner))]
    for present, device in peers:
        @pl.when(present)
        def _():
            pl.semaphore_signal(barrier, inc=1, device_id=device, device_id_type=MESH)
    n_peers = sum(present.astype(jnp.int32) for present, _ in peers)

    load_c = [pltpu.make_async_copy(c_hbm.at[e], c.at[e], sems.at[1 + e]) for e in range(3)]
    for copy in load_c:
        copy.start()

    def message(to, m):
        if m == SMALL:
            return pltpu.make_async_remote_copy(
                src_ref=ssmall, dst_ref=rsmall.at[to], send_sem=small_send.at[to], recv_sem=small_recv.at[to],
                device_id=sends_to[to], device_id_type=MESH)
        return pltpu.make_async_remote_copy(
            src_ref=sbuf.at[m], dst_ref=rbuf.at[to, m], send_sem=send_sem.at[to, m], recv_sem=recv_sem.at[to, m],
            device_id=sends_to[to], device_id_type=MESH)

    def to_passer(m):
        return pltpu.make_async_remote_copy(
            src_ref=sbuf.at[m], dst_ref=pbuf.at[m - 1], send_sem=send_sem.at[CROSS, m], recv_sem=pass_recv.at[m - 1],
            device_id=at(passer), device_id_type=MESH)

    def passed_on(m):
        return pltpu.make_async_remote_copy(
            src_ref=pbuf.at[m - 1], dst_ref=rbuf.at[CROSS, m], send_sem=pass_send.at[m - 1], recv_sem=recv_sem.at[CROSS, m],
            device_id=at(receiver), device_id_type=MESH)

    def send(m):
        if m in (0, SMALL):
            @pl.when(has_cross)
            def _():
                message(CROSS, m).start()
        else:
            @pl.when(has_cross & (m < 4 - n_passed))
            def _():
                message(CROSS, m).start()

            @pl.when(m >= 4 - n_passed)
            def _():
                to_passer(m).start()
        for to in (BELOW, PARTNER):
            @pl.when(sends[to])
            def _():
                message(to, m).start()

    def pass_on(m):
        @pl.when(m >= 4 - n_passing)
        def _():
            to_passer(m).wait_recv()
            passed_on(m).start()

    load_f.wait()
    n = n_ref[0, 0, 0]
    rows, width = 128, g.shape[1]

    def mask(i, most):
        at_rows = pl.ds(pl.multiple_of(i * rows, rows), rows)
        row, col = tri((rows, width))
        kept = jnp.where((row + i * rows < n) & (col < n), g[at_rows, :].astype(F32), 0.0)
        g[at_rows, :] = kept.astype(BF)
        return jnp.maximum(most, jnp.max(jnp.abs(kept), axis=0, keepdims=True))

    most = lax.fori_loop(0, g.shape[0] // rows, mask, jnp.zeros((1, width), F32))
    power = jnp.clip(jnp.floor(jnp.log2(jnp.maximum(most, 1e-36))), -120.0, 120.0)
    scale, inverse = jnp.exp2(power).astype(BF).astype(F32), jnp.exp2(-power).astype(BF).astype(F32)

    @pl.loop(0, g.shape[0] // rows)
    def _(i):
        at_rows = pl.ds(pl.multiple_of(i * rows, rows), rows)
        g[at_rows, :] = (g[at_rows, :].astype(F32) * inverse).astype(BF)

    h0 = gram_rows(g, 0)
    sbuf[0] = h0[:, B:3 * B].astype(BF)
    sbuf[1, :, :B] = h0[:, 3 * B:].astype(BF)
    d0 = half_diagonal(h0[:, :B])
    low0 = h0[:, :B]
    pl.semaphore_wait(barrier, n_peers)
    send(0)
    h1 = gram_rows(g, 1)
    sbuf[1, :, B:] = packed(low0, h1[:, :B]).astype(BF)
    sbuf[3] = h1[:, B:].astype(BF)
    send(1)
    h2 = gram_rows(g, 2)
    sbuf[2, :, :B] = h2[:, B:].astype(BF)
    h3 = gram_rows(g, 3)
    sbuf[2, :, B:] = packed(h2[:, :B], h3).astype(BF)
    d2 = half_diagonal(h2[:, :B])
    lines = [scale[:, 128 * p:128 * (p + 1)] for p in range(8)]
    lines += [d0[:, :128], d0[:, 128:], d2[:, :128], d2[:, 128:]]
    for p, line in enumerate(lines):
        ssmall[p:p + 1, :] = line
    ssmall[12:16, :] = jnp.zeros((4, 128), F32)
    send(SMALL)
    send(2)
    send(3)

    t_ref[...] = jnp.zeros_like(t_ref)
    for copy in load_c:
        copy.wait()

    def scale_c(frm):
        slot = slot_of[frm]
        for p in range(8):
            line = rsmall[frm, p:p + 1, :]
            column = jnp.transpose(jnp.broadcast_to(line, (128, 128)))
            at_rows = pl.ds(128 * p, 128)

            @pl.loop(0, 8)
            def _(q):
                cols = pl.ds(pl.multiple_of(q * 128, 128), 128)
                c[slot, at_rows, cols] = (c[slot, at_rows, cols].astype(F32) * column).astype(BF)

    def half_block(frm, u):
        row, col = tri((B, B))
        both = rbuf[frm, 1 if u < 2 else 2, :, B:].astype(F32)
        if u % 2 == 1:
            half[...] = jnp.where(row <= col, both, 0.0).astype(BF)
        else:
            line = jnp.concatenate([rsmall[frm, 8 + u:9 + u, :], rsmall[frm, 9 + u:10 + u, :]], axis=1)
            half[...] = jnp.where(row > col, both, jnp.where(row == col, jnp.broadcast_to(line, (B, B)), 0.0)).astype(BF)

    def consume(frm, u):
        slot = slot_of[frm]
        half_block(frm, u)
        rest = {
            0: [(rbuf.at[frm, 0], 1, 3), (rbuf.at[frm, 1, :, pl.ds(0, B)], 3, 4)],
            1: [(rbuf.at[frm, 3], 2, 4)],
            2: [(rbuf.at[frm, 2, :, pl.ds(0, B)], 3, 4)],
            3: [],
        }[u]
        for nt in range(2):
            cols = slice(512 * nt, 512 * (nt + 1))
            acc = jnp.dot(half[...], c[slot, u * B:(u + 1) * B, cols], preferred_element_type=F32)
            for factor, lo, hi in rest:
                acc += jnp.dot(factor[...], c[slot, lo * B:hi * B, cols], preferred_element_type=F32)
            z[:, cols] = acc.astype(BF)

        @pl.loop(0, 4)
        def _(i):
            cols = pl.ds(pl.multiple_of(i * B, B), B)
            t_ref[cols, :] += lax.dot_general(c[slot, u * B:(u + 1) * B, cols], z[...], TN, preferred_element_type=F32)

    def wait_for(frm, *messages):
        for m in messages:
            message(frm, m).wait_recv()

    def early(frm):
        wait_for(frm, 0, 1, SMALL)
        scale_c(frm)
        consume(frm, 0)

    def middle(frm):
        wait_for(frm, 2)
        consume(frm, 2)
        consume(frm, 3)

    def late(frm):
        wait_for(frm, 3)
        consume(frm, 1)

    early(PARTNER)
    pass_on(1)
    middle(PARTNER)
    pass_on(2)
    late(PARTNER)
    pass_on(3)

    @pl.when(has_below)
    def _():
        early(BELOW)
        middle(BELOW)

    @pl.when(has_cross)
    def _():
        early(CROSS)

    @pl.when(has_below)
    def _():
        late(BELOW)

    @pl.when(has_cross)
    def _():
        middle(CROSS)
        half_block(CROSS, 1)
        slot = slot_of[CROSS]
        right[B:, :] = c[slot, B:2 * B, :]

        @pl.loop(0, 4)
        def _(i):
            cols = pl.ds(pl.multiple_of(i * B, B), B)
            left[cols, :B] = jnp.transpose(c[slot, B:2 * B, cols])

    for gap in range(4):
        @pl.loop(0, 4 - gap)
        def _(i):
            one = pl.ds(pl.multiple_of(i * B, B), B)
            two = pl.ds(pl.multiple_of((i + gap) * B, B), B)
            upper, lower = t_ref[one, two], t_ref[two, one]
            t_ref[one, two] = upper + jnp.transpose(lower)
            if gap:
                t_ref[two, one] = lower + jnp.transpose(upper)

    @pl.when(has_cross)
    def _():
        slot = slot_of[CROSS]
        wait_for(CROSS, 3)
        for i in range(4):
            cols = slice(i * B, (i + 1) * B)
            acc = jnp.dot(half[...], c[slot, B:2 * B, cols], preferred_element_type=F32)
            acc += jnp.dot(rbuf[CROSS, 3], c[slot, 2 * B:, cols], preferred_element_type=F32)
            right[:B, cols] = acc.astype(BF)
            left[cols, B:] = jnp.transpose(acc).astype(BF)

        @pl.loop(0, 4)
        def _(i):
            cols = pl.ds(pl.multiple_of(i * B, B), B)
            t_ref[cols, :] += jnp.dot(left[cols, :], right[...], preferred_element_type=F32)

    for to in (CROSS, PARTNER, BELOW):
        @pl.when(sends[to])
        def _():
            for m in range(5):
                message(to, m).wait_send()
    for m in (1, 2, 3):
        @pl.when(m >= 4 - n_passing)
        def _():
            passed_on(m).wait_send()


def on_device(factor_inv, sep_sizes, coupling):
    width, m = factor_inv.shape[1], coupling.shape[2]
    update = pl.pallas_call(
        exchange,
        out_shape=pltpu.VMEM((m, m), F32),
        in_specs=[pl.BlockSpec(memory_space=pl.ANY), pl.BlockSpec(memory_space=pltpu.SMEM), pl.BlockSpec(memory_space=pl.ANY)],
        out_specs=pl.BlockSpec(memory_space=pltpu.VMEM),
        scratch_shapes=[
            pltpu.VMEM((width, width), BF),
            pltpu.VMEM((3, width, m), BF),
            pltpu.VMEM((B, m), BF),
            pltpu.VMEM((B, B), BF),
            pltpu.VMEM((m, 2 * B), BF),
            pltpu.VMEM((2 * B, m), BF),
            pltpu.VMEM((4, B, 2 * B), BF),
            pltpu.VMEM((16, 128), F32),
            pltpu.VMEM((3, 4, B, 2 * B), BF),
            pltpu.VMEM((3, 16, 128), F32),
            pltpu.VMEM((3, B, 2 * B), BF),
            pltpu.SemaphoreType.DMA((4,)),
            pltpu.SemaphoreType.DMA((3, 4)),
            pltpu.SemaphoreType.DMA((3, 4)),
            pltpu.SemaphoreType.DMA((3,)),
            pltpu.SemaphoreType.DMA((3,)),
            pltpu.SemaphoreType.DMA((3,)),
            pltpu.SemaphoreType.DMA((3,)),
        ],
        compiler_params=pltpu.CompilerParams(collective_id=0, has_side_effects=True, vmem_limit_bytes=48 * 1024 * 1024),
        name="exchange",
    )(factor_inv, sep_sizes, coupling)
    return update[None]


def solution(mesh):
    spec = P("gx", "gy", "gz")
    return jax.shard_map(on_device, mesh=mesh, in_specs=(spec, spec, spec), out_specs=spec, check_vma=False)
```

```python
import jax
import jax.numpy as jnp
from jax import lax
from jax.experimental import pallas as pl
from jax.experimental.pallas import tpu as pltpu
from jax.sharding import PartitionSpec as P

MESH = pl.DeviceIdType.MESH
BF = jnp.bfloat16
F32 = jnp.float32
B = 256
CROSS, PARTNER, BELOW = 0, 1, 2
SMALL = 4
TN = (((0,), (0,)), ((), ()))
NT = (((1,), (1,)), ((), ()))


def tri(shape):
    return lax.broadcasted_iota(jnp.int32, shape, 0), lax.broadcasted_iota(jnp.int32, shape, 1)


def gram(g, u, lo, hi):
    return lax.dot_general(g[:, u * B:(u + 1) * B], g[:, lo * B:hi * B], TN, preferred_element_type=F32)


def packed(lower, upper):
    row, col = tri((B, B))
    return jnp.where(row > col, lower, jnp.where(row == col, 0.5 * upper, upper))


def half_diagonal(block):
    row, col = tri((B, B))
    return jnp.sum(jnp.where(row == col, 0.5 * block, 0.0), axis=0, keepdims=True)


def exchange(f_hbm, n_hbm, c_hbm, t_ref, left, right, g, c, z, half, ct, zt, zp, n_ref, sbuf, ssmall, rbuf, rsmall, pbuf,
             f_sem, sems, send_sem, recv_sem, small_send, small_recv, pass_send, pass_recv):
    zlo, y, gz = lax.axis_index("gx"), lax.axis_index("gy"), lax.axis_index("gz")
    size_y, size_z = lax.axis_size("gy"), lax.axis_size("gz")
    core, x, kind = lax.rem(gz, 2), gz // 4, lax.rem(gz, 4)
    partner = gz + 1 - 2 * core
    cross = gz - 1 + 2 * core
    has_cross = (cross >= 0) & (cross < size_z)
    has_up, has_below = y < size_y - 1, y > 0

    steps = size_z // 4
    outer = (kind == 3) | (kind == 0)
    forward = kind == 3
    has_right, has_left = outer & (x < steps - 1), outer & (x > 0)
    n_passed = jnp.where(has_cross & outer, jnp.where(forward, x + 1, steps - x), 0)
    n_passing = jnp.where(outer, jnp.where(forward, x, steps - 1 - x), 0)
    passer = gz + jnp.where(forward, 4, -4)
    receiver = gz + jnp.where(forward, -3, 3)

    def at(col, row=None):
        row = y if row is None else jnp.clip(row, 0, size_y - 1)
        return (zlo, row, jnp.clip(col, 0, size_z - 1))

    sends_to = {CROSS: at(cross), PARTNER: at(partner), BELOW: at(gz, y + 1)}
    sends = {CROSS: has_cross, PARTNER: gz >= 0, BELOW: has_up}
    gets = {CROSS: has_cross, PARTNER: gz >= 0, BELOW: has_below}
    slot_of = {CROSS: core, PARTNER: 1 - core, BELOW: 2}

    rows, width = 128, g.shape[1]
    blocks = g.shape[0] // rows
    load_n = pltpu.make_async_copy(n_hbm, n_ref, sems.at[0])
    load_n.start()
    load_f = [pltpu.make_async_copy(f_hbm.at[0, pl.ds(rows * i, rows)], g.at[pl.ds(rows * i, rows)], f_sem.at[i]) for i in range(blocks)]
    for copy in load_f:
        copy.start()

    barrier = pltpu.get_barrier_semaphore()
    peers = [(has_cross, at(cross)), (outer, at(receiver)), (has_right, at(gz + 4)), (has_left, at(gz - 4)),
             (has_up, at(gz, y + 1)), (has_below, at(gz, y - 1)), (gz >= 0, at(partner))]
    for present, device in peers:
        @pl.when(present)
        def _():
            pl.semaphore_signal(barrier, inc=1, device_id=device, device_id_type=MESH)
    n_peers = sum(present.astype(jnp.int32) for present, _ in peers)

    load_c = [pltpu.make_async_copy(c_hbm.at[e], c.at[e], sems.at[1 + e]) for e in range(3)]

    def message(to, m):
        if m == SMALL:
            return pltpu.make_async_remote_copy(
                src_ref=ssmall, dst_ref=rsmall.at[to], send_sem=small_send.at[to], recv_sem=small_recv.at[to],
                device_id=sends_to[to], device_id_type=MESH)
        return pltpu.make_async_remote_copy(
            src_ref=sbuf.at[m], dst_ref=rbuf.at[to, m], send_sem=send_sem.at[to, m], recv_sem=recv_sem.at[to, m],
            device_id=sends_to[to], device_id_type=MESH)

    def to_passer(m):
        return pltpu.make_async_remote_copy(
            src_ref=sbuf.at[m], dst_ref=pbuf.at[m - 1], send_sem=send_sem.at[CROSS, m], recv_sem=pass_recv.at[m - 1],
            device_id=at(passer), device_id_type=MESH)

    def passed_on(m):
        return pltpu.make_async_remote_copy(
            src_ref=pbuf.at[m - 1], dst_ref=rbuf.at[CROSS, m], send_sem=pass_send.at[m - 1],
            recv_sem=recv_sem.at[CROSS, m], device_id=at(receiver), device_id_type=MESH)

    def send(m):
        if m in (0, SMALL):
            @pl.when(has_cross)
            def _():
                message(CROSS, m).start()
        else:
            @pl.when(has_cross & (m < 4 - n_passed))
            def _():
                message(CROSS, m).start()

            @pl.when(m >= 4 - n_passed)
            def _():
                to_passer(m).start()
        for to in (BELOW, PARTNER):
            @pl.when(sends[to])
            def _():
                message(to, m).start()

    def pass_on(m):
        @pl.when(m >= 4 - n_passing)
        def _():
            to_passer(m).wait_recv()
            passed_on(m).start()

    load_n.wait()
    n = n_ref[0, 0, 0]
    strip = 16

    def strip_at(i):
        return pl.ds(pl.multiple_of(i * strip, strip), strip)

    def mask_rows(i, most):
        keep = jnp.where(tri((strip, 128))[0] + i * strip < n, 1.0, 0.0).astype(BF)
        kept = g[strip_at(i), :] * jnp.concatenate([keep] * (width // 128), axis=1)
        g[strip_at(i), :] = kept
        return jnp.maximum(most, jnp.abs(kept))

    most = jnp.zeros((strip, width), BF)
    for i, copy in enumerate(load_f):
        copy.wait()
        most = lax.fori_loop(i * rows // strip, (i + 1) * rows // strip, mask_rows, most, unroll=2)
    for copy in load_c:
        copy.start()
    most = jnp.max(most.astype(F32), axis=0, keepdims=True)
    power = jnp.clip(jnp.floor(jnp.log2(jnp.maximum(most, 1e-36))), -120.0, 120.0)
    scale, inverse = jnp.exp2(power).astype(BF).astype(F32), jnp.exp2(-power)
    column = jnp.where(tri((1, width))[1] < n, inverse, 0.0)
    column = jnp.broadcast_to(column, (strip, width)).astype(BF)

    @pl.loop(0, g.shape[0] // strip, unroll=4)
    def _(i):
        g[strip_at(i), :] = g[strip_at(i), :] * column

    sbuf[0] = gram(g, 0, 1, 3).astype(BF)
    pl.semaphore_wait(barrier, n_peers)
    send(0)
    sbuf[1, :, :B] = gram(g, 0, 3, 4).astype(BF)
    low0 = gram(g, 0, 0, 1)
    d0 = half_diagonal(low0)
    h1 = gram(g, 1, 1, 4)
    sbuf[1, :, B:] = packed(low0, h1[:, :B]).astype(BF)
    sbuf[3] = h1[:, B:].astype(BF)
    h2 = gram(g, 2, 2, 4)
    sbuf[2, :, :B] = h2[:, B:].astype(BF)
    low2 = h2[:, :B]
    d2 = half_diagonal(low2)
    lines = [scale[:, 128 * p:128 * (p + 1)] for p in range(8)]
    lines += [d0[:, :128], d0[:, 128:], d2[:, :128], d2[:, 128:]]
    for p, line in enumerate(lines):
        ssmall[p:p + 1, :] = line
    ssmall[12:16, :] = jnp.zeros((4, 128), F32)
    send(SMALL)
    send(1)
    sbuf[2, :, B:] = packed(low2, gram(g, 3, 3, 4)).astype(BF)
    send(2)
    send(3)

    def scale_c(frm):
        slot = slot_of[frm]
        for p in range(8):
            line = rsmall[frm, p:p + 1, :]
            column = jnp.transpose(jnp.broadcast_to(line, (128, 128))).astype(BF)
            at_rows = pl.ds(128 * p, 128)

            @pl.loop(0, 8, unroll=4)
            def _(q):
                cols = pl.ds(pl.multiple_of(q * 128, 128), 128)
                c[slot, at_rows, cols] = c[slot, at_rows, cols] * column

    def half_block(frm, u):
        row, col = tri((B, B))
        both = rbuf[frm, 1 if u < 2 else 2, :, B:].astype(F32)
        if u % 2 == 1:
            half[...] = jnp.where(row <= col, both, 0.0).astype(BF)
        else:
            line = jnp.concatenate([rsmall[frm, 8 + u:9 + u, :], rsmall[frm, 9 + u:10 + u, :]], axis=1)
            half[...] = jnp.where(row > col, both, jnp.where(row == col, jnp.broadcast_to(line, (B, B)), 0.0)).astype(BF)

    def beside(frm, u):
        return {
            0: [(rbuf.at[frm, 0], 1, 3), (rbuf.at[frm, 1, :, pl.ds(0, B)], 3, 4)],
            1: [(rbuf.at[frm, 3], 2, 4)],
            2: [(rbuf.at[frm, 2, :, pl.ds(0, B)], 3, 4)],
            3: [],
        }[u]

    def product(frm, u):
        slot = slot_of[frm]
        half_block(frm, u)
        for nt in range(2):
            cols = slice(512 * nt, 512 * (nt + 1))
            acc = jnp.dot(half[...], c[slot, u * B:(u + 1) * B, cols], preferred_element_type=F32)
            for factor, lo, hi in beside(frm, u):
                acc += jnp.dot(factor[...], c[slot, lo * B:hi * B, cols], preferred_element_type=F32)
            z[u * B:(u + 1) * B, cols] = acc.astype(BF)

    def product_t(u):
        half_block(CROSS, u)
        for i in range(4):
            rows_i = slice(i * B, (i + 1) * B)
            acc = lax.dot_general(ct[rows_i, u * B:(u + 1) * B], half[...], NT, preferred_element_type=F32)
            for factor, lo, hi in beside(CROSS, u):
                acc += lax.dot_general(ct[rows_i, lo * B:hi * B], factor[...], NT, preferred_element_type=F32)
            zt[rows_i, u * B:(u + 1) * B] = acc.astype(BF)

    def wait_for(frm, *messages):
        for m in messages:
            message(frm, m).wait_recv()

    def prepare(frm):
        wait_for(frm, 0, SMALL, 1)
        scale_c(frm)
        product(frm, 0)

    def add_up(frm, first):
        slot = slot_of[frm]

        @pl.loop(0, 4)
        def _(i):
            cols = pl.ds(pl.multiple_of(i * B, B), B)
            added = lax.dot_general(c[slot, :, cols], z[...], TN, preferred_element_type=F32)
            t_ref[cols, :] = added if first else t_ref[cols, :] + added

    for copy in load_c:
        copy.wait()
    prepare(PARTNER)
    wait_for(PARTNER, 2)
    product(PARTNER, 2)
    product(PARTNER, 3)
    pass_on(1)
    wait_for(PARTNER, 3)
    product(PARTNER, 1)
    pass_on(2)
    add_up(PARTNER, True)
    pass_on(3)

    @pl.when(has_cross)
    def _():
        wait_for(CROSS, 0, SMALL)
        scale_c(CROSS)
        slot = slot_of[CROSS]

        @pl.loop(0, 4)
        def _(k):
            block = pl.ds(pl.multiple_of(k * B, B), B)
            for i in range(4):
                ct[i * B:(i + 1) * B, block] = jnp.transpose(c[slot, block, i * B:(i + 1) * B])

    @pl.when(has_below)
    def _():
        prepare(BELOW)
        wait_for(BELOW, 2)
        product(BELOW, 2)
        product(BELOW, 3)
        wait_for(BELOW, 3)
        product(BELOW, 1)
        add_up(BELOW, False)

    @pl.when(has_cross)
    def _():
        wait_for(CROSS, 1)
        product_t(0)

        @pl.loop(0, 4)
        def _(i):
            cols = pl.ds(pl.multiple_of(i * B, B), B)
            t_ref[cols, :] += lax.dot_general(ct[cols, :B], zt[:, :B], NT, preferred_element_type=F32)

        half_block(CROSS, 1)
        for i in range(4):
            rows_i = slice(i * B, (i + 1) * B)
            zp[rows_i, :] = lax.dot_general(ct[rows_i, B:2 * B], half[...], NT, preferred_element_type=F32)

    for gap in range(4):
        @pl.loop(0, 4 - gap)
        def _(i):
            one = pl.ds(pl.multiple_of(i * B, B), B)
            two = pl.ds(pl.multiple_of((i + gap) * B, B), B)
            upper, lower = t_ref[one, two], t_ref[two, one]
            t_ref[one, two] = upper + jnp.transpose(lower)
            if gap:
                t_ref[two, one] = lower + jnp.transpose(upper)

    @pl.when(has_cross)
    def _():
        wait_for(CROSS, 2)
        product_t(2)
        product_t(3)

        @pl.loop(0, 4)
        def _(i):
            cols = pl.ds(pl.multiple_of(i * B, B), B)
            added = lax.dot_general(ct[cols, 2 * B:], zt[:, 2 * B:], NT, preferred_element_type=F32)
            added += lax.dot_general(zt[cols, 2 * B:], ct[:, 2 * B:], NT, preferred_element_type=F32)
            t_ref[cols, :] += added

    @pl.when(has_cross)
    def _():
        left[:, :B] = ct[:, B:2 * B]
        right[:, B:] = ct[:, B:2 * B]
        wait_for(CROSS, 3)
        for i in range(4):
            cols = slice(i * B, (i + 1) * B)
            acc = zp[cols, :] + lax.dot_general(ct[cols, 2 * B:], rbuf[CROSS, 3], NT, preferred_element_type=F32)
            acc = acc.astype(BF)
            left[cols, B:] = acc
            right[cols, :B] = acc

    @pl.when(jnp.logical_not(has_cross))
    def _():
        left[...] = jnp.zeros_like(left)
        right[...] = jnp.zeros_like(right)

    for to in (CROSS, PARTNER, BELOW):
        @pl.when(sends[to])
        def _():
            for m in range(5):
                message(to, m).wait_send()
    for m in (1, 2, 3):
        @pl.when(m >= 4 - n_passing)
        def _():
            passed_on(m).wait_send()


def last_part(t_ref, left, right, s_hbm, s, sems):
    tile = s.shape[1] // sems.shape[0]
    copies = []
    for i in range(sems.shape[0]):
        at = pl.ds(i * tile, tile)
        s[:, at] = t_ref[:, at] + lax.dot_general(left[...], right[at, :], NT, preferred_element_type=F32)
        copies.append(pltpu.make_async_copy(s.at[:, at], s_hbm.at[0, :, at], sems.at[i]))
        copies[-1].start()
    for copy in copies:
        copy.wait()


def on_device(factor_inv, sep_sizes, coupling):
    width, m = factor_inv.shape[1], coupling.shape[2]
    parts = pl.pallas_call(
        exchange,
        out_shape=(pltpu.VMEM((m, m), F32), pltpu.VMEM((m, 2 * B), BF), pltpu.VMEM((m, 2 * B), BF)),
        in_specs=[pl.BlockSpec(memory_space=pltpu.HBM)] * 3,
        out_specs=(pl.BlockSpec(memory_space=pltpu.VMEM),) * 3,
        scratch_shapes=[
            pltpu.VMEM((width, width), BF),
            pltpu.VMEM((3, width, m), BF),
            pltpu.VMEM((width, m), BF),
            pltpu.VMEM((B, B), BF),
            pltpu.VMEM((m, width), BF),
            pltpu.VMEM((m, width), BF),
            pltpu.VMEM((m, B), F32),
            pltpu.SMEM((1, 1, 1), jnp.int32),
            pltpu.VMEM((4, B, 2 * B), BF),
            pltpu.VMEM((16, 128), F32),
            pltpu.VMEM((3, 4, B, 2 * B), BF),
            pltpu.VMEM((3, 16, 128), F32),
            pltpu.VMEM((3, B, 2 * B), BF),
            pltpu.SemaphoreType.DMA((8,)),
            pltpu.SemaphoreType.DMA((4,)),
            pltpu.SemaphoreType.DMA((3, 4)),
            pltpu.SemaphoreType.DMA((3, 4)),
            pltpu.SemaphoreType.DMA((3,)),
            pltpu.SemaphoreType.DMA((3,)),
            pltpu.SemaphoreType.DMA((4,)),
            pltpu.SemaphoreType.DMA((4,)),
        ],
        compiler_params=pltpu.CompilerParams(collective_id=0, has_side_effects=True, vmem_limit_bytes=54 * 1024 * 1024),
        name="exchange",
    )(factor_inv, sep_sizes, coupling)
    return pl.pallas_call(
        last_part,
        out_shape=jax.ShapeDtypeStruct((1, m, m), F32),
        in_specs=[pl.BlockSpec(memory_space=pltpu.VMEM)] * 3,
        out_specs=pl.BlockSpec(memory_space=pl.ANY),
        scratch_shapes=[pltpu.VMEM((m, m), F32), pltpu.SemaphoreType.DMA((4,))],
        compiler_params=pltpu.CompilerParams(vmem_limit_bytes=8 * 1024 * 1024),
        name="last_part",
    )(*parts)


def solution(mesh):
    spec = P("gx", "gy", "gz")
    return jax.shard_map(on_device, mesh=mesh, in_specs=(spec, spec, spec), out_specs=spec, check_vma=False)
```

```python
import jax
import jax.numpy as jnp
from jax import lax
from jax.experimental import pallas as pl
from jax.experimental.pallas import tpu as pltpu
from jax.sharding import PartitionSpec as P

MESH = pl.DeviceIdType.MESH
BF = jnp.bfloat16
F32 = jnp.float32
B = 256
CROSS, PARTNER, BELOW = 0, 1, 2
SMALL = 4
TN = (((0,), (0,)), ((), ()))
NT = (((1,), (1,)), ((), ()))


def tri(shape):
    return lax.broadcasted_iota(jnp.int32, shape, 0), lax.broadcasted_iota(jnp.int32, shape, 1)


def gram(g, u, lo, hi):
    return lax.dot_general(g[:, u * B:(u + 1) * B], g[:, lo * B:hi * B], TN, preferred_element_type=F32)


def packed(lower, upper):
    row, col = tri((B, B))
    return jnp.where(row > col, lower, jnp.where(row == col, 0.5 * upper, upper))


def half_diagonal(block):
    row, col = tri((B, B))
    return jnp.sum(jnp.where(row == col, 0.5 * block, 0.0), axis=0, keepdims=True)


def exchange(f_hbm, n_hbm, c_hbm, t_ref, left, right, g, c, z, half, ct, zt, zp, n_ref, sbuf, ssmall, rbuf, rsmall, pbuf,
             f_sem, sems, send_sem, recv_sem, small_send, small_recv, pass_send, pass_recv):
    zlo, y, gz = lax.axis_index("gx"), lax.axis_index("gy"), lax.axis_index("gz")
    size_y, size_z = lax.axis_size("gy"), lax.axis_size("gz")
    core, x, kind = lax.rem(gz, 2), gz // 4, lax.rem(gz, 4)
    partner = gz + 1 - 2 * core
    cross = gz - 1 + 2 * core
    has_cross = (cross >= 0) & (cross < size_z)
    has_up, has_below = y < size_y - 1, y > 0

    steps = size_z // 4
    outer = (kind == 3) | (kind == 0)
    forward = kind == 3
    has_right, has_left = outer & (x < steps - 1), outer & (x > 0)
    n_passed = jnp.where(has_cross & outer, jnp.where(forward, x + 1, steps - x), 0)
    n_passing = jnp.where(outer, jnp.where(forward, x, steps - 1 - x), 0)
    passer = gz + jnp.where(forward, 4, -4)
    receiver = gz + jnp.where(forward, -3, 3)

    def at(col, row=None):
        row = y if row is None else jnp.clip(row, 0, size_y - 1)
        return (zlo, row, jnp.clip(col, 0, size_z - 1))

    sends_to = {CROSS: at(cross), PARTNER: at(partner), BELOW: at(gz, y + 1)}
    sends = {CROSS: has_cross, PARTNER: gz >= 0, BELOW: has_up}
    gets = {CROSS: has_cross, PARTNER: gz >= 0, BELOW: has_below}
    slot_of = {CROSS: core, PARTNER: 1 - core, BELOW: 2}

    rows, width = 128, g.shape[1]
    blocks = g.shape[0] // rows
    load_n = pltpu.make_async_copy(n_hbm, n_ref, sems.at[0])
    load_n.start()
    load_f = [pltpu.make_async_copy(f_hbm.at[0, pl.ds(rows * i, rows)], g.at[pl.ds(rows * i, rows)], f_sem.at[i]) for i in range(blocks)]
    for copy in load_f:
        copy.start()

    barrier = pltpu.get_barrier_semaphore()
    peers = [(has_cross, at(cross)), (outer, at(receiver)), (has_right, at(gz + 4)), (has_left, at(gz - 4)),
             (has_up, at(gz, y + 1)), (has_below, at(gz, y - 1)), (gz >= 0, at(partner))]
    for present, device in peers:
        @pl.when(present)
        def _():
            pl.semaphore_signal(barrier, inc=1, device_id=device, device_id_type=MESH)
    n_peers = sum(present.astype(jnp.int32) for present, _ in peers)

    load_c = [pltpu.make_async_copy(c_hbm.at[e], c.at[e], sems.at[1 + e]) for e in range(3)]

    def message(to, m):
        if m == SMALL:
            return pltpu.make_async_remote_copy(
                src_ref=ssmall, dst_ref=rsmall.at[to], send_sem=small_send.at[to], recv_sem=small_recv.at[to],
                device_id=sends_to[to], device_id_type=MESH)
        return pltpu.make_async_remote_copy(
            src_ref=sbuf.at[m], dst_ref=rbuf.at[to, m], send_sem=send_sem.at[to, m], recv_sem=recv_sem.at[to, m],
            device_id=sends_to[to], device_id_type=MESH)

    def to_passer(m):
        return pltpu.make_async_remote_copy(
            src_ref=sbuf.at[m], dst_ref=pbuf.at[m - 1], send_sem=send_sem.at[CROSS, m], recv_sem=pass_recv.at[m - 1],
            device_id=at(passer), device_id_type=MESH)

    def passed_on(m):
        return pltpu.make_async_remote_copy(
            src_ref=pbuf.at[m - 1], dst_ref=rbuf.at[CROSS, m], send_sem=pass_send.at[m - 1],
            recv_sem=recv_sem.at[CROSS, m], device_id=at(receiver), device_id_type=MESH)

    def send(m):
        if m in (0, SMALL):
            @pl.when(has_cross)
            def _():
                message(CROSS, m).start()
        else:
            @pl.when(has_cross & (m < 4 - n_passed))
            def _():
                message(CROSS, m).start()

            @pl.when(m >= 4 - n_passed)
            def _():
                to_passer(m).start()
        for to in (BELOW, PARTNER):
            @pl.when(sends[to])
            def _():
                message(to, m).start()

    def pass_on(m):
        @pl.when(m >= 4 - n_passing)
        def _():
            to_passer(m).wait_recv()
            passed_on(m).start()

    load_n.wait()
    n = n_ref[0, 0, 0]
    strip = 16

    def strip_at(i):
        return pl.ds(pl.multiple_of(i * strip, strip), strip)

    def mask_rows(i, most):
        keep = jnp.where(tri((strip, 128))[0] + i * strip < n, 1.0, 0.0).astype(BF)
        kept = g[strip_at(i), :] * jnp.concatenate([keep] * (width // 128), axis=1)
        g[strip_at(i), :] = kept
        return jnp.maximum(most, jnp.abs(kept))

    most = jnp.zeros((strip, width), BF)
    for i, copy in enumerate(load_f):
        copy.wait()
        most = lax.fori_loop(i * rows // strip, (i + 1) * rows // strip, mask_rows, most, unroll=2)
    for copy in load_c:
        copy.start()
    most = jnp.max(most.astype(F32), axis=0, keepdims=True)
    power = jnp.clip(jnp.floor(jnp.log2(jnp.maximum(most, 1e-36))), -120.0, 120.0)
    scale, inverse = jnp.exp2(power).astype(BF).astype(F32), jnp.exp2(-power)
    column = jnp.where(tri((1, width))[1] < n, inverse, 0.0)
    column = jnp.broadcast_to(column, (strip, width)).astype(BF)

    def scale_g(cols):
        @pl.loop(0, g.shape[0] // strip, unroll=4)
        def _(i):
            g[strip_at(i), cols] = g[strip_at(i), cols] * column[:, cols]

    scale_g(slice(0, 3 * B))
    sbuf[0] = gram(g, 0, 1, 3).astype(BF)
    pl.semaphore_wait(barrier, n_peers)
    send(0)
    scale_g(slice(3 * B, width))
    sbuf[1, :, :B] = gram(g, 0, 3, 4).astype(BF)
    low0 = gram(g, 0, 0, 1)
    d0 = half_diagonal(low0)
    h1 = gram(g, 1, 1, 4)
    sbuf[1, :, B:] = packed(low0, h1[:, :B]).astype(BF)
    sbuf[3] = h1[:, B:].astype(BF)
    h2 = gram(g, 2, 2, 4)
    sbuf[2, :, :B] = h2[:, B:].astype(BF)
    low2 = h2[:, :B]
    d2 = half_diagonal(low2)
    lines = [scale[:, 128 * p:128 * (p + 1)] for p in range(8)]
    lines += [d0[:, :128], d0[:, 128:], d2[:, :128], d2[:, 128:]]
    ssmall[...] = jnp.concatenate(lines + [jnp.zeros((4, 128), F32)], axis=0).astype(BF)
    send(SMALL)
    send(1)
    sbuf[2, :, B:] = packed(low2, gram(g, 3, 3, 4)).astype(BF)
    send(2)
    send(3)

    def scale_c(frm):
        slot = slot_of[frm]
        lines = rsmall[frm].astype(F32)
        for p in range(8):
            line = lines[p:p + 1, :]
            column = jnp.transpose(jnp.broadcast_to(line, (128, 128))).astype(BF)
            at_rows = pl.ds(128 * p, 128)

            @pl.loop(0, 8, unroll=4)
            def _(q):
                cols = pl.ds(pl.multiple_of(q * 128, 128), 128)
                c[slot, at_rows, cols] = c[slot, at_rows, cols] * column

    def half_block(frm, u):
        row, col = tri((B, B))
        both = rbuf[frm, 1 if u < 2 else 2, :, B:].astype(F32)
        if u % 2 == 1:
            half[...] = jnp.where(row <= col, both, 0.0).astype(BF)
        else:
            lines = rsmall[frm].astype(F32)
            line = jnp.concatenate([lines[8 + u:9 + u, :], lines[9 + u:10 + u, :]], axis=1)
            half[...] = jnp.where(row > col, both, jnp.where(row == col, jnp.broadcast_to(line, (B, B)), 0.0)).astype(BF)

    def beside(frm, u):
        return {
            0: [(rbuf.at[frm, 0], 1, 3), (rbuf.at[frm, 1, :, pl.ds(0, B)], 3, 4)],
            1: [(rbuf.at[frm, 3], 2, 4)],
            2: [(rbuf.at[frm, 2, :, pl.ds(0, B)], 3, 4)],
            3: [],
        }[u]

    def product(frm, u):
        slot = slot_of[frm]
        half_block(frm, u)
        for nt in range(2):
            cols = slice(512 * nt, 512 * (nt + 1))
            acc = jnp.dot(half[...], c[slot, u * B:(u + 1) * B, cols], preferred_element_type=F32)
            for factor, lo, hi in beside(frm, u):
                acc += jnp.dot(factor[...], c[slot, lo * B:hi * B, cols], preferred_element_type=F32)
            z[u * B:(u + 1) * B, cols] = acc.astype(BF)

    def product_t(u):
        half_block(CROSS, u)
        for i in range(4):
            rows_i = slice(i * B, (i + 1) * B)
            acc = lax.dot_general(ct[rows_i, u * B:(u + 1) * B], half[...], NT, preferred_element_type=F32)
            for factor, lo, hi in beside(CROSS, u):
                acc += lax.dot_general(ct[rows_i, lo * B:hi * B], factor[...], NT, preferred_element_type=F32)
            zt[rows_i, u * B:(u + 1) * B] = acc.astype(BF)

    def wait_for(frm, *messages):
        for m in messages:
            message(frm, m).wait_recv()

    def prepare(frm):
        wait_for(frm, 0, SMALL, 1)
        scale_c(frm)
        product(frm, 0)

    def add_up(frm, first):
        slot = slot_of[frm]

        @pl.loop(0, 4)
        def _(i):
            cols = pl.ds(pl.multiple_of(i * B, B), B)
            added = lax.dot_general(c[slot, :, cols], z[...], TN, preferred_element_type=F32)
            t_ref[cols, :] = added if first else t_ref[cols, :] + added

    for copy in load_c:
        copy.wait()
    prepare(PARTNER)
    wait_for(PARTNER, 2)
    product(PARTNER, 2)
    product(PARTNER, 3)
    pass_on(1)
    wait_for(PARTNER, 3)
    product(PARTNER, 1)
    pass_on(2)
    add_up(PARTNER, True)
    pass_on(3)

    @pl.when(has_cross)
    def _():
        wait_for(CROSS, 0, SMALL)
        scale_c(CROSS)
        slot = slot_of[CROSS]

        @pl.loop(0, 4)
        def _(k):
            block = pl.ds(pl.multiple_of(k * B, B), B)
            for i in range(4):
                ct[i * B:(i + 1) * B, block] = jnp.transpose(c[slot, block, i * B:(i + 1) * B])

    @pl.when(has_below)
    def _():
        prepare(BELOW)
        wait_for(BELOW, 2)
        product(BELOW, 2)
        product(BELOW, 3)
        wait_for(BELOW, 3)
        product(BELOW, 1)
        add_up(BELOW, False)

    @pl.when(has_cross)
    def _():
        wait_for(CROSS, 1)
        product_t(0)

        @pl.loop(0, 4)
        def _(i):
            cols = pl.ds(pl.multiple_of(i * B, B), B)
            t_ref[cols, :] += lax.dot_general(ct[cols, :B], zt[:, :B], NT, preferred_element_type=F32)

        half_block(CROSS, 1)
        for i in range(4):
            rows_i = slice(i * B, (i + 1) * B)
            zp[rows_i, :] = lax.dot_general(ct[rows_i, B:2 * B], half[...], NT, preferred_element_type=F32)

    for gap in range(4):
        @pl.loop(0, 4 - gap)
        def _(i):
            one = pl.ds(pl.multiple_of(i * B, B), B)
            two = pl.ds(pl.multiple_of((i + gap) * B, B), B)
            upper, lower = t_ref[one, two], t_ref[two, one]
            t_ref[one, two] = upper + jnp.transpose(lower)
            if gap:
                t_ref[two, one] = lower + jnp.transpose(upper)

    @pl.when(has_cross)
    def _():
        wait_for(CROSS, 2)
        product_t(2)
        product_t(3)

        @pl.loop(0, 4)
        def _(i):
            cols = pl.ds(pl.multiple_of(i * B, B), B)
            added = lax.dot_general(ct[cols, 2 * B:], zt[:, 2 * B:], NT, preferred_element_type=F32)
            added += lax.dot_general(zt[cols, 2 * B:], ct[:, 2 * B:], NT, preferred_element_type=F32)
            t_ref[cols, :] += added

    @pl.when(has_cross)
    def _():
        left[:, :B] = ct[:, B:2 * B]
        right[:, B:] = ct[:, B:2 * B]
        wait_for(CROSS, 3)
        for i in range(4):
            cols = slice(i * B, (i + 1) * B)
            acc = zp[cols, :] + lax.dot_general(ct[cols, 2 * B:], rbuf[CROSS, 3], NT, preferred_element_type=F32)
            acc = acc.astype(BF)
            left[cols, B:] = acc
            right[cols, :B] = acc

    @pl.when(jnp.logical_not(has_cross))
    def _():
        left[...] = jnp.zeros_like(left)
        right[...] = jnp.zeros_like(right)

    for to in (CROSS, PARTNER, BELOW):
        @pl.when(sends[to])
        def _():
            for m in range(5):
                message(to, m).wait_send()
    for m in (1, 2, 3):
        @pl.when(m >= 4 - n_passing)
        def _():
            passed_on(m).wait_send()


def last_part(t_ref, left, right, s_hbm, s, sems):
    tile = s.shape[0] // sems.shape[0]
    copies = []
    for i in range(sems.shape[0]):
        at = pl.ds(i * tile, tile)
        s[at, :] = t_ref[at, :] + lax.dot_general(left[at, :], right[...], NT, preferred_element_type=F32)
        copies.append(pltpu.make_async_copy(s.at[at], s_hbm.at[0, at], sems.at[i]))
        copies[-1].start()
    for copy in copies:
        copy.wait()


def on_device(factor_inv, sep_sizes, coupling):
    width, m = factor_inv.shape[1], coupling.shape[2]
    parts = pl.pallas_call(
        exchange,
        out_shape=(pltpu.VMEM((m, m), F32), pltpu.VMEM((m, 2 * B), BF), pltpu.VMEM((m, 2 * B), BF)),
        in_specs=[pl.BlockSpec(memory_space=pltpu.HBM)] * 3,
        out_specs=(pl.BlockSpec(memory_space=pltpu.VMEM),) * 3,
        scratch_shapes=[
            pltpu.VMEM((width, width), BF),
            pltpu.VMEM((3, width, m), BF),
            pltpu.VMEM((width, m), BF),
            pltpu.VMEM((B, B), BF),
            pltpu.VMEM((m, width), BF),
            pltpu.VMEM((m, width), BF),
            pltpu.VMEM((m, B), F32),
            pltpu.SMEM((1, 1, 1), jnp.int32),
            pltpu.VMEM((4, B, 2 * B), BF),
            pltpu.VMEM((16, 128), BF),
            pltpu.VMEM((3, 4, B, 2 * B), BF),
            pltpu.VMEM((3, 16, 128), BF),
            pltpu.VMEM((3, B, 2 * B), BF),
            pltpu.SemaphoreType.DMA((8,)),
            pltpu.SemaphoreType.DMA((4,)),
            pltpu.SemaphoreType.DMA((3, 4)),
            pltpu.SemaphoreType.DMA((3, 4)),
            pltpu.SemaphoreType.DMA((3,)),
            pltpu.SemaphoreType.DMA((3,)),
            pltpu.SemaphoreType.DMA((4,)),
            pltpu.SemaphoreType.DMA((4,)),
        ],
        compiler_params=pltpu.CompilerParams(collective_id=0, has_side_effects=True, vmem_limit_bytes=54 * 1024 * 1024),
        name="exchange",
    )(factor_inv, sep_sizes, coupling)
    return pl.pallas_call(
        last_part,
        out_shape=jax.ShapeDtypeStruct((1, m, m), F32),
        in_specs=[pl.BlockSpec(memory_space=pltpu.VMEM)] * 3,
        out_specs=pl.BlockSpec(memory_space=pl.ANY),
        scratch_shapes=[pltpu.VMEM((m, m), F32), pltpu.SemaphoreType.DMA((4,))],
        compiler_params=pltpu.CompilerParams(vmem_limit_bytes=8 * 1024 * 1024),
        name="last_part",
    )(*parts)


def solution(mesh):
    spec = P("gx", "gy", "gz")
    return jax.shard_map(on_device, mesh=mesh, in_specs=(spec, spec, spec), out_specs=spec, check_vma=False)
```

```python
import jax
import jax.numpy as jnp
from jax import lax
from jax.experimental import pallas as pl
from jax.experimental.pallas import tpu as pltpu
from jax.sharding import PartitionSpec as P

MESH = pl.DeviceIdType.MESH
BF = jnp.bfloat16
F32 = jnp.float32
B = 256
CROSS, PARTNER, BELOW = 0, 1, 2
SMALL = 4
TN = (((0,), (0,)), ((), ()))
NT = (((1,), (1,)), ((), ()))


def tri(shape):
    return lax.broadcasted_iota(jnp.int32, shape, 0), lax.broadcasted_iota(jnp.int32, shape, 1)


def gram(g, u, lo, hi):
    return lax.dot_general(g[:, u * B:(u + 1) * B], g[:, lo * B:hi * B], TN, preferred_element_type=F32)


def packed(lower, upper):
    row, col = tri((B, B))
    return jnp.where(row > col, lower, jnp.where(row == col, 0.5 * upper, upper))


def half_diagonal(block):
    row, col = tri((B, B))
    return jnp.sum(jnp.where(row == col, 0.5 * block, 0.0), axis=0, keepdims=True)


def exchange(f_hbm, n_hbm, c_hbm, t_ref, left, right, g, c, z, half, ct, zt, zp, n_ref, sbuf, ssmall, rbuf, rsmall, pbuf,
             f_sem, sems, send_sem, recv_sem, small_send, small_recv, pass_send, pass_recv):
    zlo, y, gz = lax.axis_index("gx"), lax.axis_index("gy"), lax.axis_index("gz")
    size_y, size_z = lax.axis_size("gy"), lax.axis_size("gz")
    core, x, kind = lax.rem(gz, 2), gz // 4, lax.rem(gz, 4)
    partner = gz + 1 - 2 * core
    cross = gz - 1 + 2 * core
    has_cross = (cross >= 0) & (cross < size_z)
    has_up, has_below = y < size_y - 1, y > 0

    steps = size_z // 4
    outer = (kind == 3) | (kind == 0)
    forward = kind == 3
    has_right, has_left = outer & (x < steps - 1), outer & (x > 0)
    n_passed = jnp.where(has_cross & outer, jnp.where(forward, x + 1, steps - x), 0)
    n_passing = jnp.where(outer, jnp.where(forward, x, steps - 1 - x), 0)
    passer = gz + jnp.where(forward, 4, -4)
    receiver = gz + jnp.where(forward, -3, 3)

    def at(col, row=None):
        row = y if row is None else jnp.clip(row, 0, size_y - 1)
        return (zlo, row, jnp.clip(col, 0, size_z - 1))

    sends_to = {CROSS: at(cross), PARTNER: at(partner), BELOW: at(gz, y + 1)}
    sends = {CROSS: has_cross, PARTNER: gz >= 0, BELOW: has_up}
    gets = {CROSS: has_cross, PARTNER: gz >= 0, BELOW: has_below}
    slot_of = {CROSS: core, PARTNER: 1 - core, BELOW: 2}

    rows, width = 128, g.shape[1]
    blocks = g.shape[0] // rows
    load_n = pltpu.make_async_copy(n_hbm, n_ref, sems.at[0])
    load_n.start()
    load_f = [pltpu.make_async_copy(f_hbm.at[0, pl.ds(rows * i, rows)], g.at[pl.ds(rows * i, rows)], f_sem.at[i]) for i in range(blocks)]
    for copy in load_f:
        copy.start()

    barrier = pltpu.get_barrier_semaphore()
    peers = [(has_cross, at(cross)), (outer, at(receiver)), (has_right, at(gz + 4)), (has_left, at(gz - 4)),
             (has_up, at(gz, y + 1)), (has_below, at(gz, y - 1)), (gz >= 0, at(partner))]
    for present, device in peers:
        @pl.when(present)
        def _():
            pl.semaphore_signal(barrier, inc=1, device_id=device, device_id_type=MESH)
    n_peers = sum(present.astype(jnp.int32) for present, _ in peers)

    load_c = [pltpu.make_async_copy(c_hbm.at[e], c.at[e], sems.at[1 + e]) for e in range(3)]

    def message(to, m):
        if m == SMALL:
            return pltpu.make_async_remote_copy(
                src_ref=ssmall, dst_ref=rsmall.at[to], send_sem=small_send.at[to], recv_sem=small_recv.at[to],
                device_id=sends_to[to], device_id_type=MESH)
        return pltpu.make_async_remote_copy(
            src_ref=sbuf.at[m], dst_ref=rbuf.at[to, m], send_sem=send_sem.at[to, m], recv_sem=recv_sem.at[to, m],
            device_id=sends_to[to], device_id_type=MESH)

    def to_passer(m):
        return pltpu.make_async_remote_copy(
            src_ref=sbuf.at[m], dst_ref=pbuf.at[m - 1], send_sem=send_sem.at[CROSS, m], recv_sem=pass_recv.at[m - 1],
            device_id=at(passer), device_id_type=MESH)

    def passed_on(m):
        return pltpu.make_async_remote_copy(
            src_ref=pbuf.at[m - 1], dst_ref=rbuf.at[CROSS, m], send_sem=pass_send.at[m - 1],
            recv_sem=recv_sem.at[CROSS, m], device_id=at(receiver), device_id_type=MESH)

    def send(m):
        if m in (0, SMALL):
            @pl.when(has_cross)
            def _():
                message(CROSS, m).start()
        else:
            @pl.when(has_cross & (m < 4 - n_passed))
            def _():
                message(CROSS, m).start()

            @pl.when(m >= 4 - n_passed)
            def _():
                to_passer(m).start()
        for to in (BELOW, PARTNER):
            @pl.when(sends[to])
            def _():
                message(to, m).start()

    def pass_on(m):
        @pl.when(m >= 4 - n_passing)
        def _():
            to_passer(m).wait_recv()
            passed_on(m).start()

    load_n.wait()
    n = n_ref[0, 0, 0]
    strip = 16

    def strip_at(i):
        return pl.ds(pl.multiple_of(i * strip, strip), strip)

    def mask_rows(i, most):
        keep = jnp.where(tri((strip, 128))[0] + i * strip < n, 1.0, 0.0).astype(BF)
        kept = g[strip_at(i), :] * jnp.concatenate([keep] * (width // 128), axis=1)
        g[strip_at(i), :] = kept
        return jnp.maximum(most, jnp.abs(kept))

    most = jnp.zeros((strip, width), BF)
    for i, copy in enumerate(load_f):
        copy.wait()
        most = lax.fori_loop(i * rows // strip, (i + 1) * rows // strip, mask_rows, most, unroll=8)
    for copy in load_c:
        copy.start()
    most = jnp.max(most.astype(F32), axis=0, keepdims=True)
    power = jnp.clip(jnp.floor(jnp.log2(jnp.maximum(most, 1e-36))), -120.0, 120.0)
    scale, inverse = jnp.exp2(power).astype(BF).astype(F32), jnp.exp2(-power)
    column = jnp.where(tri((1, width))[1] < n, inverse, 0.0)
    column = jnp.broadcast_to(column, (strip, width)).astype(BF)

    def scale_g(cols):
        @pl.loop(0, g.shape[0] // strip, unroll=16)
        def _(i):
            g[strip_at(i), cols] = g[strip_at(i), cols] * column[:, cols]

    scale_g(slice(0, 3 * B))
    sbuf[0] = gram(g, 0, 1, 3).astype(BF)
    pl.semaphore_wait(barrier, n_peers)
    send(0)
    scale_g(slice(3 * B, width))
    sbuf[1, :, :B] = gram(g, 0, 3, 4).astype(BF)
    low0 = gram(g, 0, 0, 1)
    d0 = half_diagonal(low0)
    h1 = gram(g, 1, 1, 4)
    sbuf[1, :, B:] = packed(low0, h1[:, :B]).astype(BF)
    sbuf[3] = h1[:, B:].astype(BF)
    h2 = gram(g, 2, 2, 4)
    sbuf[2, :, :B] = h2[:, B:].astype(BF)
    low2 = h2[:, :B]
    d2 = half_diagonal(low2)
    lines = [scale[:, 128 * p:128 * (p + 1)] for p in range(8)]
    lines += [d0[:, :128], d0[:, 128:], d2[:, :128], d2[:, 128:]]
    ssmall[...] = jnp.concatenate(lines + [jnp.zeros((4, 128), F32)], axis=0).astype(BF)
    send(SMALL)
    send(1)
    sbuf[2, :, B:] = packed(low2, gram(g, 3, 3, 4)).astype(BF)
    send(2)
    send(3)

    def scale_c(frm):
        slot = slot_of[frm]
        lines = rsmall[frm].astype(F32)
        for p in range(8):
            line = lines[p:p + 1, :]
            column = jnp.transpose(jnp.broadcast_to(line, (128, 128))).astype(BF)
            at_rows = pl.ds(128 * p, 128)

            @pl.loop(0, 8, unroll=4)
            def _(q):
                cols = pl.ds(pl.multiple_of(q * 128, 128), 128)
                c[slot, at_rows, cols] = c[slot, at_rows, cols] * column

    def half_block(frm, u):
        row, col = tri((B, B))
        both = rbuf[frm, 1 if u < 2 else 2, :, B:].astype(F32)
        if u % 2 == 1:
            half[...] = jnp.where(row <= col, both, 0.0).astype(BF)
        else:
            lines = rsmall[frm].astype(F32)
            line = jnp.concatenate([lines[8 + u:9 + u, :], lines[9 + u:10 + u, :]], axis=1)
            half[...] = jnp.where(row > col, both, jnp.where(row == col, jnp.broadcast_to(line, (B, B)), 0.0)).astype(BF)

    def beside(frm, u):
        return {
            0: [(rbuf.at[frm, 0], 1, 3), (rbuf.at[frm, 1, :, pl.ds(0, B)], 3, 4)],
            1: [(rbuf.at[frm, 3], 2, 4)],
            2: [(rbuf.at[frm, 2, :, pl.ds(0, B)], 3, 4)],
            3: [],
        }[u]

    def product(frm, u):
        slot = slot_of[frm]
        half_block(frm, u)
        for nt in range(2):
            cols = slice(512 * nt, 512 * (nt + 1))
            acc = jnp.dot(half[...], c[slot, u * B:(u + 1) * B, cols], preferred_element_type=F32)
            for factor, lo, hi in beside(frm, u):
                acc += jnp.dot(factor[...], c[slot, lo * B:hi * B, cols], preferred_element_type=F32)
            z[u * B:(u + 1) * B, cols] = acc.astype(BF)

    def product_t(u):
        half_block(CROSS, u)
        for i in range(4):
            rows_i = slice(i * B, (i + 1) * B)
            acc = lax.dot_general(ct[rows_i, u * B:(u + 1) * B], half[...], NT, preferred_element_type=F32)
            for factor, lo, hi in beside(CROSS, u):
                acc += lax.dot_general(ct[rows_i, lo * B:hi * B], factor[...], NT, preferred_element_type=F32)
            zt[rows_i, u * B:(u + 1) * B] = acc.astype(BF)

    def wait_for(frm, *messages):
        for m in messages:
            message(frm, m).wait_recv()

    def prepare(frm):
        wait_for(frm, 0, SMALL, 1)
        scale_c(frm)
        product(frm, 0)

    def add_up(frm, first):
        slot = slot_of[frm]

        @pl.loop(0, 4)
        def _(i):
            cols = pl.ds(pl.multiple_of(i * B, B), B)
            added = lax.dot_general(c[slot, :, cols], z[...], TN, preferred_element_type=F32)
            t_ref[cols, :] = added if first else t_ref[cols, :] + added

    for copy in load_c:
        copy.wait()
    prepare(PARTNER)
    wait_for(PARTNER, 2)
    product(PARTNER, 2)
    product(PARTNER, 3)
    pass_on(1)
    wait_for(PARTNER, 3)
    product(PARTNER, 1)
    pass_on(2)
    add_up(PARTNER, True)
    pass_on(3)

    @pl.when(has_cross)
    def _():
        wait_for(CROSS, 0, SMALL)
        scale_c(CROSS)
        slot = slot_of[CROSS]

        @pl.loop(0, 4)
        def _(k):
            block = pl.ds(pl.multiple_of(k * B, B), B)
            for i in range(4):
                ct[i * B:(i + 1) * B, block] = jnp.transpose(c[slot, block, i * B:(i + 1) * B])

    @pl.when(has_below)
    def _():
        prepare(BELOW)
        wait_for(BELOW, 2)
        product(BELOW, 2)
        product(BELOW, 3)
        wait_for(BELOW, 3)
        product(BELOW, 1)
        add_up(BELOW, False)

    @pl.when(has_cross)
    def _():
        wait_for(CROSS, 1)
        product_t(0)

        @pl.loop(0, 4)
        def _(i):
            cols = pl.ds(pl.multiple_of(i * B, B), B)
            t_ref[cols, :] += lax.dot_general(ct[cols, :B], zt[:, :B], NT, preferred_element_type=F32)

        half_block(CROSS, 1)
        for i in range(4):
            rows_i = slice(i * B, (i + 1) * B)
            zp[rows_i, :] = lax.dot_general(ct[rows_i, B:2 * B], half[...], NT, preferred_element_type=F32)

    for gap in range(4):
        @pl.loop(0, 4 - gap)
        def _(i):
            one = pl.ds(pl.multiple_of(i * B, B), B)
            two = pl.ds(pl.multiple_of((i + gap) * B, B), B)
            upper, lower = t_ref[one, two], t_ref[two, one]
            t_ref[one, two] = upper + jnp.transpose(lower)
            if gap:
                t_ref[two, one] = lower + jnp.transpose(upper)

    @pl.when(has_cross)
    def _():
        wait_for(CROSS, 2)
        product_t(2)
        product_t(3)

        @pl.loop(0, 4)
        def _(i):
            cols = pl.ds(pl.multiple_of(i * B, B), B)
            added = lax.dot_general(ct[cols, 2 * B:], zt[:, 2 * B:], NT, preferred_element_type=F32)
            added += lax.dot_general(zt[cols, 2 * B:], ct[:, 2 * B:], NT, preferred_element_type=F32)
            t_ref[cols, :] += added

    @pl.when(has_cross)
    def _():
        left[:, :B] = ct[:, B:2 * B]
        right[:, B:] = ct[:, B:2 * B]
        wait_for(CROSS, 3)
        for i in range(4):
            cols = slice(i * B, (i + 1) * B)
            acc = zp[cols, :] + lax.dot_general(ct[cols, 2 * B:], rbuf[CROSS, 3], NT, preferred_element_type=F32)
            acc = acc.astype(BF)
            left[cols, B:] = acc
            right[cols, :B] = acc

    @pl.when(jnp.logical_not(has_cross))
    def _():
        left[...] = jnp.zeros_like(left)
        right[...] = jnp.zeros_like(right)

    for to in (CROSS, PARTNER, BELOW):
        @pl.when(sends[to])
        def _():
            for m in range(5):
                message(to, m).wait_send()
    for m in (1, 2, 3):
        @pl.when(m >= 4 - n_passing)
        def _():
            passed_on(m).wait_send()


def last_part(t_ref, left, right, s_hbm, s, sems):
    tile = s.shape[0] // sems.shape[0]
    copies = []
    for i in range(sems.shape[0]):
        at = pl.ds(i * tile, tile)
        s[at, :] = t_ref[at, :] + lax.dot_general(left[at, :], right[...], NT, preferred_element_type=F32)
        copies.append(pltpu.make_async_copy(s.at[at], s_hbm.at[0, at], sems.at[i]))
        copies[-1].start()
    for copy in copies:
        copy.wait()


def on_device(factor_inv, sep_sizes, coupling):
    width, m = factor_inv.shape[1], coupling.shape[2]
    parts = pl.pallas_call(
        exchange,
        out_shape=(pltpu.VMEM((m, m), F32), pltpu.VMEM((m, 2 * B), BF), pltpu.VMEM((m, 2 * B), BF)),
        in_specs=[pl.BlockSpec(memory_space=pltpu.HBM)] * 3,
        out_specs=(pl.BlockSpec(memory_space=pltpu.VMEM),) * 3,
        scratch_shapes=[
            pltpu.VMEM((width, width), BF),
            pltpu.VMEM((3, width, m), BF),
            pltpu.VMEM((width, m), BF),
            pltpu.VMEM((B, B), BF),
            pltpu.VMEM((m, width), BF),
            pltpu.VMEM((m, width), BF),
            pltpu.VMEM((m, B), F32),
            pltpu.SMEM((1, 1, 1), jnp.int32),
            pltpu.VMEM((4, B, 2 * B), BF),
            pltpu.VMEM((16, 128), BF),
            pltpu.VMEM((3, 4, B, 2 * B), BF),
            pltpu.VMEM((3, 16, 128), BF),
            pltpu.VMEM((3, B, 2 * B), BF),
            pltpu.SemaphoreType.DMA((8,)),
            pltpu.SemaphoreType.DMA((4,)),
            pltpu.SemaphoreType.DMA((3, 4)),
            pltpu.SemaphoreType.DMA((3, 4)),
            pltpu.SemaphoreType.DMA((3,)),
            pltpu.SemaphoreType.DMA((3,)),
            pltpu.SemaphoreType.DMA((4,)),
            pltpu.SemaphoreType.DMA((4,)),
        ],
        compiler_params=pltpu.CompilerParams(collective_id=0, has_side_effects=True, vmem_limit_bytes=54 * 1024 * 1024),
        name="exchange",
    )(factor_inv, sep_sizes, coupling)
    return pl.pallas_call(
        last_part,
        out_shape=jax.ShapeDtypeStruct((1, m, m), F32),
        in_specs=[pl.BlockSpec(memory_space=pltpu.VMEM)] * 3,
        out_specs=pl.BlockSpec(memory_space=pl.ANY),
        scratch_shapes=[pltpu.VMEM((m, m), F32), pltpu.SemaphoreType.DMA((4,))],
        compiler_params=pltpu.CompilerParams(vmem_limit_bytes=8 * 1024 * 1024),
        name="last_part",
    )(*parts)


def solution(mesh):
    spec = P("gx", "gy", "gz")
    return jax.shard_map(on_device, mesh=mesh, in_specs=(spec, spec, spec), out_specs=spec, check_vma=False)
```
